32 devices in a mesh: gx: 8 (over y, x, core), gy: 4 (over z).
Axes of the slice: x: 2, y: 2, z: 4, core: 2. Of those that a mesh axis runs over, the one named last changes fastest.
Arguments:
- collocation: bfloat16 [3072, 16384], P(None, 'gx'), may hold values from -6 to 6
- density: bfloat16 [3072, 3072], P('gy'), may hold values from -0.109375 to 0.109375
- kernel: bfloat16 [16384, 8, 4, 512], P('gx', None, 'gy'), may hold values from -6.67572e-06 to 6.67572e-06
Outputs:
- exchange: float32 [3072, 3072], P('gx', 'gy')
The draws below stay inside these ranges and needn't reach their ends.
All inputs are finite; a program needn't handle non-finite values.
Results may differ from the reference program's by a relative error of at most 0.008.
Values may be sent and summed in bfloat16 or wider, within the bound.
A program may use at most 448 MiB of HBM per device.

```python
import jax
import jax.numpy as jnp
from jax import lax

NBF = 3072
NPTS = 16384
CYCLE_LEN = 8
COL_GROUPS = 4
PIECE = 512
N_GX = 8


def block_levels(stream_key, shape, pieces, smallest, high):
    factor_of, own = 1.0, jax.random.fold_in(stream_key, 6)
    for dim, blocks in pieces:
        steps = jnp.exp(jax.random.uniform(jax.random.fold_in(own, dim), (blocks,), jnp.float32, smallest / len(pieces), high / len(pieces)))
        factor_of = factor_of * jnp.repeat(steps, shape[dim] // blocks).reshape([-1 if axis == dim else 1 for axis in range(len(shape))])
    return factor_of


def noise(rng, shape, deviation, limit, cuts=(), held_as=jnp.bfloat16):
    values = deviation * jax.random.normal(rng, shape, jnp.float32)
    if cuts:
        values = values * block_levels(rng, shape, cuts, -0.22, 0.18)
    return jnp.clip(values, -limit, limit).astype(held_as)


def setup_inputs(seed: int = 0) -> dict:
    key_list = jax.random.split(jax.random.key(seed), 4)
    collocation = noise(key_list[0], (NBF, NPTS), 1.0, 6.0, ((1, 8),))
    density = noise(key_list[1], (NBF, NBF), NBF ** -0.5, 0.109375, ((0, 4),))
    kernel = noise(key_list[2], (NPTS, CYCLE_LEN, COL_GROUPS, PIECE), (NPTS * NPTS * NBF) ** -0.5, 6.67572021484375e-06, ((0, 8), (2, 4)))
    return {"collocation": collocation, "density": density, "kernel": kernel}


def reference(collocation, density, kernel):
    dense = jnp.dot(density, collocation, preferred_element_type=jnp.float32).astype(jnp.bfloat16)
    flat_kernel = kernel.reshape(NPTS, NPTS)
    block_len = NPTS // N_GX

    def scan_step(running, position):
        offset = (position * block_len).astype(jnp.int32)
        dense_rows = lax.dynamic_slice_in_dim(dense, offset, block_len, 1)
        colloc_rows = lax.dynamic_slice_in_dim(collocation, offset, block_len, 1)
        coefficients = lax.dynamic_slice_in_dim(flat_kernel, offset, block_len, 0)
        products = jnp.dot(dense_rows.T, collocation, preferred_element_type=jnp.float32)
        weighted = (coefficients.astype(jnp.float32) * products).astype(jnp.bfloat16)
        contracted = jnp.dot(weighted, collocation.T, preferred_element_type=jnp.float32).astype(jnp.bfloat16)
        return running + jnp.dot(colloc_rows, contracted, preferred_element_type=jnp.float32), None

    running, unused = lax.scan(scan_step, jnp.zeros((NBF, NBF), jnp.float32), jnp.arange(N_GX, dtype=jnp.int32))
    return running
```

```python
import jax
import jax.numpy as jnp
from jax import lax
from jax.sharding import PartitionSpec as P

F32 = jnp.float32
BF16 = jnp.bfloat16


def spread(block, axis_size, axis):
    rows = block.shape[0]
    me = lax.axis_index("gy")
    out = jnp.zeros((axis_size * rows, block.shape[1]), block.dtype)
    out = lax.dynamic_update_slice_in_dim(out, block, me * rows, 0)
    for shift in range(1, axis_size):
        pairs = [(k, (k + shift) % axis_size) for k in range(axis_size)]
        got = lax.ppermute(block, axis, pairs)
        source = lax.rem(me + axis_size - shift, axis_size)
        out = lax.dynamic_update_slice_in_dim(out, got, source * rows, 0)
    return out


def exchange_sum(part, axis_size, axis):
    width = part.shape[1] // axis_size
    me = lax.axis_index(axis)
    total = lax.dynamic_slice_in_dim(part, me * width, width, 1).astype(F32)
    for shift in range(1, axis_size):
        pairs = [(k, (k + shift) % axis_size) for k in range(axis_size)]
        target = lax.rem(me + shift, axis_size)
        sent = lax.dynamic_slice_in_dim(part, target * width, width, 1)
        total = total + lax.ppermute(sent, axis, pairs).astype(F32)
    return total


def build(n_gx, n_gy):
    def local(collocation, density, kernel):
        nbf, panel_rows = collocation.shape
        piece = kernel.shape[3]
        i, j = lax.axis_index("gx"), lax.axis_index("gy")
        halves = 2 if piece % 256 == 0 else 1
        half = piece // halves
        own = [
            lax.dynamic_slice_in_dim(collocation, j * piece + h * half, half, 1)
            for h in range(halves)
        ]
        gathered = [lax.all_gather(own[0], "gx", axis=1, tiled=True)]

        cols = nbf // n_gx
        strip = spread(lax.dynamic_slice_in_dim(density, i * cols, cols, 1), n_gy, "gy")
        whole = lax.all_gather(strip, "gx", axis=0, tiled=False)
        for h in range(1, halves):
            later, whole = lax.optimization_barrier((own[h], whole))
            gathered.append(lax.all_gather(later, "gx", axis=1, tiled=True))
        dense = lax.dot_general(
            whole,
            collocation.reshape(n_gx, cols, panel_rows),
            (((0, 2), (0, 1)), ((), ())),
            preferred_element_type=F32,
        ).astype(BF16)

        weighted = []
        for h in range(halves):
            tile = kernel[:, :, 0, h * half : (h + 1) * half].reshape(panel_rows, -1)
            products = lax.dot_general(
                dense, gathered[h], (((0,), (0,)), ((), ())), preferred_element_type=F32
            )
            weighted.append((tile.astype(F32) * products).astype(BF16))

        parts = 3 if (nbf // n_gy) % 384 == 0 else 1
        sub = nbf // n_gy // parts
        done = []
        for c in range(parts):
            contracted = 0.0
            for h in range(halves):
                rows = gathered[h].reshape(n_gy, parts, sub, -1)[:, c].reshape(n_gy * sub, -1)
                contracted = contracted + lax.dot_general(
                    rows, weighted[h], (((1,), (1,)), ((), ())), preferred_element_type=F32
                )
            term = lax.dot_general(
                collocation,
                contracted.astype(BF16),
                (((1,), (1,)), ((), ())),
                preferred_element_type=F32,
            ).astype(BF16)
            summed = lax.psum_scatter(term, "gx", scatter_dimension=0, tiled=True)
            done.append(exchange_sum(summed, n_gy, "gy"))
        return jnp.concatenate(done, axis=1)

    return local


def solution(mesh):
    return jax.shard_map(
        build(mesh.shape["gx"], mesh.shape["gy"]),
        mesh=mesh,
        in_specs=(P(None, "gx"), P("gy", None), P("gx", None, "gy", None)),
        out_specs=P("gx", "gy"),
        check_vma=False,
    )
```
